128 devices in a mesh: dp: 8 (over y, z_lo), section: 16 (over z_hi, x, core).
Axes of the slice: x: 4, y: 4, z: 4 (z_hi: 2, z_lo: 2; z = z_hi * 2 + z_lo), core: 2. Of those that a mesh axis runs over, the one named last changes fastest.
Arguments:
- inputs: bfloat16 [2, 1024, 2048], P(None, 'dp'), may hold values from -6 to 6
- cotangent: bfloat16 [2, 1024, 2048], P(None, 'dp'), may hold values from -6 to 6
- w_prev: float32 [16, 2048, 2048], P('section', None, 'dp'), may hold values from -6 to 6
- w_now: float32 [16, 2048, 2048], P('section', None, 'dp'), may hold values from -6 to 6
- grads_prev: bfloat16 [8, 16, 2048, 2048], P('dp', 'section'), may hold values from -6 to 6
Outputs:
- w_next: float32 [16, 2048, 2048], P('section', None, 'dp')
- grads_next: bfloat16 [8, 16, 2048, 2048], P('dp', 'section')
The draws below stay inside these ranges and needn't reach their ends.
All inputs are finite; a program needn't handle non-finite values.
Results may differ from the reference program's by a relative error of at most 0.02.
Values may be sent and summed in bfloat16 or wider, within the bound.
No kernel may reach another device: no remote copies, remote signals or barrier semaphores. Data moves between devices by JAX's collectives and lax.ppermute only.
A program may use at most 128 MiB of HBM per device.

```python
import jax
import jax.numpy as jnp
from jax import lax

D = 2048
MB = 2
TOKENS = 1024
SECTIONS = 16
N_DP = 8


def raised(drawn, stream_key, source, target, parts, factor):
    owner, partner = [(jnp.arange(drawn.shape[axis_at]) // (drawn.shape[axis_at] // parts)).reshape([-1 if axis == axis_at else 1 for axis in range(drawn.ndim)]) for axis_at in (source, target)]
    chosen = jax.random.permutation(stream_key, parts)[partner]
    strong = (owner == chosen) | (owner == (partner + parts // 2) % parts)
    return jnp.where(strong, factor * drawn, drawn)


def levels(stream_key, shape, pieces, least, top_value):
    def one(dim, shards_of):
        steps = jax.random.uniform(jax.random.fold_in(jax.random.fold_in(stream_key, 6), dim), (shards_of,), jnp.float32, least / len(pieces), top_value / len(pieces))
        return jnp.repeat(jnp.exp(steps), shape[dim] // shards_of).reshape((-1,) + (1,) * (len(shape) - dim - 1))

    gain = one(*pieces[0])
    for cut in pieces[1:]:
        gain = gain * one(*cut)
    return gain


def bell_draw(key, dims, deviation, most, shards=(), kind=jnp.bfloat16):
    factor_of = levels(key, dims, shards, -0.22, 0.18) if shards else 1.0
    values = jax.random.normal(key, dims, jnp.float32) * deviation * factor_of
    return jnp.minimum(jnp.maximum(values, -most), most).astype(kind)


def noise_with(own_key, dims, spread, most, shards, heavy, dtype=jnp.bfloat16):
    array = spread * jax.random.normal(own_key, dims, jnp.float32)
    if shards:
        array = array * levels(own_key, dims, shards, -0.22, 0.18)
    return jnp.clip(raised(array, jax.random.fold_in(own_key, 3), *heavy), -most, most).astype(dtype)


def setup_inputs(seed: int = 0) -> dict:
    key_list = jax.random.split(jax.random.key(seed), 6)
    return {
        "inputs": bell_draw(key_list[0], (MB, TOKENS, D), 1.0, 6.0, ((1, 8),)),
        "cotangent": bell_draw(key_list[1], (MB, TOKENS, D), 1.0, 6.0, ((1, 8),)),
        "w_prev": bell_draw(key_list[2], (SECTIONS, D, D), 1.0, 6.0, ((0, 16), (2, 8)), jnp.float32),
        "w_now": bell_draw(key_list[3], (SECTIONS, D, D), 1.0, 6.0, ((0, 16), (2, 8)), jnp.float32),
        "grads_prev": noise_with(key_list[4], (N_DP, SECTIONS, D, D), 0.5, 6.0, ((0, 8), (1, 16)), (0, 3, 8, 2.0)),
    }


norm_eps = 1e-06
learn_rate = 1.0

def section_parts(x_bf, weight_bf):
    width = weight_bf.shape[0]
    inv = width ** (-0.5)
    x = x_bf.astype(jnp.float32)
    scale = lax.rsqrt(lax.optimization_barrier(jnp.mean(x * x, axis=-1, keepdims=True)) + norm_eps)
    normed = x * scale
    upper = normed.astype(jnp.bfloat16)
    pre = jnp.dot(upper.reshape(-1, width), weight_bf, preferred_element_type=jnp.float32).reshape(x.shape) * inv
    return (x, scale, normed, upper, pre)

def reference(inputs, cotangent, w_prev, w_now, grads_prev):
    n_rep = grads_prev.shape[0]
    sections = w_prev.shape[0]
    width = w_prev.shape[1]
    inv = width ** (-0.5)
    micro = inputs.shape[0]
    tok_mb = inputs.shape[1] // n_rep
    acts = inputs
    saved = []
    for s in range(sections):
        weight_bf = w_prev[s].astype(jnp.bfloat16)
        saved.append(acts)
        x, scale, normed, upper, pre = section_parts(acts, weight_bf)
        acts = (x + jax.nn.silu(pre)).astype(jnp.bfloat16)
    back = cotangent
    grads = [None] * sections
    for s in reversed(range(sections)):
        weight_bf = w_prev[s].astype(jnp.bfloat16)
        x, scale, normed, upper, pre = section_parts(saved[s], weight_bf)
        dy = back.astype(jnp.float32)
        sig = jax.nn.sigmoid(pre)
        dpre = dy * sig * (1.0 + pre * (1.0 - sig))
        small = (dpre * inv).astype(jnp.bfloat16)
        du = jnp.dot(small.reshape(-1, width), weight_bf.T, preferred_element_type=jnp.float32).reshape(x.shape)
        dx = dy + scale * (du - normed * lax.optimization_barrier(jnp.mean(du * normed, axis=-1, keepdims=True)))
        back = dx.astype(jnp.bfloat16)
        upper_r = upper.reshape(micro, n_rep, tok_mb, width).astype(jnp.float32)
        small_r = small.reshape(micro, n_rep, tok_mb, width).astype(jnp.float32)
        grads[s] = jnp.einsum('mrtd,mrte->rde', upper_r, small_r).astype(jnp.bfloat16)
    grads_next = jnp.stack(grads, axis=1)
    total = jnp.zeros(w_now.shape, jnp.float32)
    for rep in range(n_rep):
        total = total + grads_prev[rep].astype(jnp.float32)
    w_next = w_now - learn_rate * total / n_rep
    return (w_next, grads_next)
```

```python
import functools

import jax
import jax.numpy as jnp
from jax import lax
from jax.experimental import pallas as pl
from jax.experimental.pallas import tpu as pltpu
from jax.sharding import PartitionSpec as P


EPS = 1e-06
LEARN_RATE = 1.0
CHUNKS = 4
SKEW = 2
PAIR = 2
F32 = jnp.float32
BF16 = jnp.bfloat16


def dot(a, b):
    return jnp.dot(a, b, preferred_element_type=F32)


def assemble_kernel(info, *refs):
    mine, other, out, sems = refs[:9], refs[9:18], refs[18], refs[-1]
    core = info[0]
    copies = []
    for slot, blocks in ((core, mine), (1 - core, other)):
        row = out.at[slot]
        for at, block in zip((0, 2, 4, 6, 8, 10, 11, 12, 14), blocks):
            copies.append((block, row.at[pl.ds(at, block.shape[0])]))
    started = [pltpu.make_async_copy(s, d, sems.at[i]) for i, (s, d) in enumerate(copies)]
    for copy in started:
        copy.start()
    for copy in started:
        copy.wait()


def transpose_kernel(w_in, w):
    del w_in
    n_blk, _, blk = w.shape[1:]

    def swap(l, j, k):
        at_j, at_k = (pl.ds(pl.multiple_of(v * blk, blk), blk) for v in (j, k))
        upper, lower = w[l, j, at_k, :], w[l, k, at_j, :]
        w[l, j, at_k, :] = lower.T
        w[l, k, at_j, :] = upper.T

    @pl.loop(0, PAIR)
    def _(l):
        for j in range(n_blk):
            rows = slice(j * blk, (j + 1) * blk)
            w[l, j, rows, :] = w[l, j, rows, :].T

        @pl.loop(1, n_blk // 2)
        def _(d):
            for j in range(n_blk):
                swap(l, j, lax.rem(j + d, n_blk))

        for j in range(n_blk // 2):
            swap(l, j, j + n_blk // 2)


def forward_kernel(tick, info, x_in, inp, w, su_i, sx_i, sd_i, sr_i, y, su, sx, sd, sr):
    del su_i, sx_i, sd_i, sr_i
    n_blk, width, blk = w.shape[1:]
    inv = width ** (-0.5)
    place = info[1]
    chunk = tick - SKEW * place

    @pl.when((chunk >= 0) & (chunk < CHUNKS))
    def _():
        @pl.when(place == 0)
        def _():
            y[...] = inp[chunk]

        @pl.when(place != 0)
        def _():
            y[...] = x_in[...]

        @pl.loop(0, PAIR)
        def _(l):
            xb = y[...]
            x = xb.astype(F32)
            scale = lax.rsqrt(jnp.mean(x * x, axis=-1, keepdims=True) + EPS)
            sx[l, chunk] = xb
            sr[l, chunk] = jnp.broadcast_to(scale, sr.shape[2:])
            su[l, chunk] = (x * scale).astype(BF16)

            @pl.loop(0, 2)
            def _(part):
                for i in range(n_blk // 2):
                    j = part * (n_blk // 2) + i
                    cols = pl.ds(pl.multiple_of(info[2 + j], blk), blk)
                    z = dot(su[l, chunk], w[l, j]) * inv
                    sg = jax.nn.sigmoid(z)
                    sd[l, chunk, :, pl.ds(pl.multiple_of(j * blk, blk), blk)] = sg * (1.0 + z * (1.0 - sg)) * inv
                    y[:, cols] = (sx[l, chunk, :, cols].astype(F32) + z * sg).astype(BF16)


def backward_kernel(tick, stages, info, g_in, cot, w, sx, sd, sr, sq_i, dx, sq, qrel, du):
    del sq_i
    n_blk, width, blk = w.shape[1:]
    place = stages - 1 - info[1]
    chunk = tick - SKEW * place

    @pl.when((chunk >= 0) & (chunk < CHUNKS))
    def _():
        @pl.when(place == 0)
        def _():
            dx[...] = cot[chunk]

        @pl.when(place != 0)
        def _():
            dx[...] = g_in[...]

        @pl.loop(0, PAIR)
        def _(step):
            l = PAIR - 1 - step
            for j in range(n_blk):
                cols = pl.ds(pl.multiple_of(info[2 + j], blk), blk)
                q = (dx[:, cols].astype(F32) * sd[l, chunk, :, j * blk : (j + 1) * blk]).astype(BF16)
                qrel[:, j * blk : (j + 1) * blk] = q
                sq[l, chunk, :, cols] = q

            @pl.loop(0, 2)
            def _(part):
                for i in range(n_blk // 2):
                    k = part * (n_blk // 2) + i
                    du[:, pl.ds(pl.multiple_of(k * blk, blk), blk)] = dot(qrel[...], w[l, k])

            scale = sr[l, chunk][:, :1]
            n = sx[l, chunk].astype(F32) * scale
            g = du[...]
            back = dx[...].astype(F32) + scale * (g - n * jnp.mean(g * n, axis=-1, keepdims=True))
            dx[...] = back.astype(BF16)


def pack_kernel(info, su, sq, out):
    other = 1 - info[0]
    out[0] = su[other]
    out[1] = sq[other]


def gradient_kernel(info, su, sq, recv, out):
    core = info[0]
    depth, width = out.shape
    cols = pl.ds(pl.multiple_of(pl.program_id(0) * depth, depth), depth)
    tokens = lambda v: v.reshape(-1, v.shape[-1])
    u = jnp.concatenate([tokens(su[core, :, :, cols]), tokens(recv[0, :, :, cols])], 0)
    for k in range(0, width, 512):
        q = jnp.concatenate([tokens(sq[core, :, :, k : k + 512]), tokens(recv[1, :, :, k : k + 512])], 0)
        part = lax.dot_general(u, q, (((0,), (0,)), ((), ())), preferred_element_type=F32)
        out[:, k : k + 512] = part.astype(BF16)


VM = pl.BlockSpec(memory_space=pltpu.VMEM)
SM = pl.BlockSpec(memory_space=pltpu.SMEM)
HB = pl.BlockSpec(memory_space=pltpu.HBM)


def cost(flops):
    return pl.CostEstimate(flops=flops, bytes_accessed=0, transcendentals=0)


def params(mib):
    return pltpu.CompilerParams(vmem_limit_bytes=mib * 1024 * 1024)


def body(inputs, cotangent, w_prev, w_now, grads_prev):
    n_dp = lax.axis_size("dp")
    n_sec = lax.axis_size("section")
    stages = n_sec // PAIR
    micro, tok_mb, width = inputs.shape
    blk = w_prev.shape[2]
    rows = tok_mb // CHUNKS
    sec = lax.axis_index("section")
    core = sec % PAIR
    stage = sec // PAIR
    dp = lax.axis_index("dp")
    n_y = n_dp // 2

    def over_dp(move):
        pairs = []
        for y in range(n_y):
            for z in range(2):
                ty, tz = move(y, z)
                pairs.append((2 * y + z, 2 * (ty % n_y) + tz))
        return lambda v: lax.ppermute(v, "dp", pairs)

    swap_z = over_dp(lambda y, z: (y, 1 - z))
    to_up = over_dp(lambda y, z: (y + 1, z))
    to_down = over_dp(lambda y, z: (y - 1, z))
    swap_core = lambda v: lax.ppermute(v, "section", [(s, s ^ 1) for s in range(n_sec)])

    lanes = blk // 2
    own = w_prev[0].astype(BF16).reshape(width, 2, lanes).transpose(1, 0, 2)
    zo, below, above, own_o = lax.optimization_barrier((swap_z(own), to_up(own), to_down(own), swap_core(own)))
    above_z, below_z, far, zo_o, below_o, above_o = lax.optimization_barrier(
        (swap_z(above), to_up(zo), to_down(above), swap_core(zo), swap_core(below), swap_core(above))
    )
    far_za, far_zb, above_zo, below_zo, far_o = lax.optimization_barrier(
        (to_up(below_z[:1]), to_down(above_z[1:]), swap_core(above_z), swap_core(below_z), swap_core(far))
    )
    mine = (own, zo, above, above_z, far, far_za, far_zb, below, below_z)
    y_at, z_at = dp // 2, dp % 2
    rel = [(0, 0), (0, 1), (1, 0), (1, 1), (2, 0), (2, 1), (n_y - 1, 0), (n_y - 1, 1)]
    off = [(((y_at + dy) % n_y) * 2 + (z_at + dz) % 2) * blk + h * lanes for dy, dz in rel for h in range(2)]
    info = jnp.stack([core, stage] + off).astype(jnp.int32)
    pick = lambda v, at: lax.dynamic_index_in_dim(v, at, 0, keepdims=False)
    inp = pick(inputs, core).reshape(CHUNKS, rows, width)
    cot = pick(cotangent, core).reshape(CHUNKS, rows, width)
    far_zao, far_zbo, gp, inp, cot, info = lax.optimization_barrier(
        (swap_core(far_za), swap_core(far_zb), grads_prev, inp, cot, info)
    )
    other = (own_o, zo_o, above_o, above_zo, far_o, far_zao, far_zbo, below_o, below_zo)

    shares = lax.psum_scatter(gp[0, 0], "dp", scatter_dimension=1, tiled=True)

    saved = (PAIR, CHUNKS, rows, width)
    w_res, su, sx, sd, sr, sq, first = pl.pallas_call(
        assemble_kernel,
        out_shape=[
            pltpu.VMEM((PAIR, 2 * n_dp, width, lanes), BF16),
            pltpu.VMEM(saved, BF16),
            pltpu.VMEM(saved, BF16),
            pltpu.VMEM(saved, F32),
            pltpu.VMEM((PAIR, CHUNKS, rows, 128), F32),
            pltpu.VMEM(saved, BF16),
            pltpu.VMEM((rows, width), BF16),
        ],
        in_specs=[SM] + [HB] * 18,
        out_specs=[VM] * 7,
        scratch_shapes=[pltpu.SemaphoreType.DMA((18,))],
        compiler_params=params(1),
        name="assemble",
    )(info, *[pltpu.with_memory_space_constraint(v, pltpu.HBM) for v in mine + other])

    def transposed(w):
        return pl.pallas_call(
            transpose_kernel,
            out_shape=pltpu.VMEM(w.shape, w.dtype),
            in_specs=[VM],
            out_specs=VM,
            input_output_aliases={0: 0},
            compiler_params=params(1),
            name="transpose",
        )(w)

    def forward_call(tick, *args):
        return pl.pallas_call(
            functools.partial(forward_kernel, tick),
            out_shape=[
                pltpu.VMEM((rows, width), BF16),
                pltpu.VMEM(su.shape, su.dtype),
                pltpu.VMEM(sx.shape, sx.dtype),
                pltpu.VMEM(sd.shape, sd.dtype),
                pltpu.VMEM(sr.shape, sr.dtype),
            ],
            in_specs=[SM] + [VM] * 7,
            out_specs=[VM] * 5,
            input_output_aliases={4: 1, 5: 2, 6: 3, 7: 4},
            compiler_params=params(1),
            cost_estimate=cost(PAIR * 2 * rows * width * width),
            name="forward",
        )(info, *args)

    def backward_call(tick, *args):
        return pl.pallas_call(
            functools.partial(backward_kernel, tick, stages),
            out_shape=[pltpu.VMEM((rows, width), BF16), pltpu.VMEM(sq.shape, sq.dtype)],
            in_specs=[SM] + [VM] * 7,
            out_specs=[VM] * 2,
            scratch_shapes=[pltpu.VMEM((rows, width), BF16), pltpu.VMEM((rows, width), F32)],
            input_output_aliases={7: 1},
            compiler_params=params(1),
            cost_estimate=cost(PAIR * 2 * rows * width * width),
            name="backward",
        )(info, *args)

    ticks = SKEW * (stages - 1) + CHUNKS

    def hop(value, tick, step):
        pairs = []
        for p in range(stages - 1):
            if 0 <= tick - SKEW * p < CHUNKS:
                a, b = (p, p + 1) if step > 0 else (stages - 1 - p, stages - 2 - p)
                pairs += [(PAIR * a + c, PAIR * b + c) for c in range(PAIR)]
        return lax.ppermute(value, "section", pairs) if pairs else None

    def relay(step, call):
        arrived = {}
        for tick in range(ticks):
            arrived[tick] = hop(call(tick, arrived.get(tick - SKEW)), tick, step)

    state = [w_res, su, sx, sd, sr, sq]

    def forward(tick, arrived):
        x_in = first if arrived is None else arrived
        y, *state[1:5] = forward_call(tick, x_in, inp, *state[:5])
        return y

    def backward(tick, arrived):
        g_in = first if arrived is None else arrived
        g, state[5] = backward_call(tick, g_in, cot, state[0], *state[2:6])
        return g

    relay(1, forward)
    state[0] = transposed(state[0])
    relay(-1, backward)
    su, sq = state[1], state[5]

    packed = pl.pallas_call(
        pack_kernel,
        out_shape=pltpu.VMEM((2,) + saved[1:], BF16),
        in_specs=[SM, VM, VM],
        out_specs=VM,
        compiler_params=params(1),
        name="pack",
    )(info, su, sq)
    dweight = pl.pallas_call(
        gradient_kernel,
        grid=(width // 256,),
        out_shape=jax.ShapeDtypeStruct((width, width), BF16),
        in_specs=[SM] + [VM] * 3,
        out_specs=pl.BlockSpec((256, width), lambda i: (i, 0)),
        compiler_params=params(8),
        cost_estimate=cost(4 * tok_mb * width * width),
        name="gradient",
    )(info, su, sq, swap_core(packed))
    grads_next = dweight[None, None]
    w_next = w_now - LEARN_RATE / n_dp * shares.astype(F32)[None]
    return (w_next, grads_next)


def solution(mesh):
    placed = (
        P(None, "dp", None),
        P(None, "dp", None),
        P("section", None, "dp"),
        P("section", None, "dp"),
        P("dp", "section", None, None),
    )
    return jax.shard_map(
        body,
        mesh=mesh,
        in_specs=placed,
        out_specs=(P("section", None, "dp"), P("dp", "section", None, None)),
        check_vma=False,
    )
```

```python
import functools

import jax
import jax.numpy as jnp
from jax import lax
from jax.experimental import pallas as pl
from jax.experimental.pallas import tpu as pltpu
from jax.sharding import PartitionSpec as P


EPS = 1e-06
LEARN_RATE = 1.0
CHUNKS = 4
SKEW = 2
PAIR = 2
F32 = jnp.float32
BF16 = jnp.bfloat16


def dot(a, b):
    return jnp.dot(a, b, preferred_element_type=F32)


def copy_all(pairs, sems):
    started = [pltpu.make_async_copy(s, d, sems.at[i]) for i, (s, d) in enumerate(pairs)]
    for copy in started:
        copy.start()
    for copy in started:
        copy.wait()


def assemble_kernel(info, *refs):
    w, sems = refs[18], refs[-1]
    pairs = []
    for slot, blocks in ((info[0], refs[:9]), (1 - info[0], refs[9:18])):
        row = w.at[slot]
        for at, block in zip((0, 2, 4, 6, 8, 10, 11, 12, 14), blocks):
            pairs.append((block, row.at[pl.ds(at, block.shape[0])]))
    copy_all(pairs, sems)


def transpose_kernel(early, stages, info, w, *refs):
    t, buf, sems = refs[-3:]
    n_blk, _, blk = w.shape[1:]
    mine = info[1] * 2 >= stages if early else info[1] * 2 < stages
    steps = PAIR * n_blk

    def copy(i, slot):
        return pltpu.make_async_copy(buf.at[slot], t.at[lax.div(i, n_blk), lax.rem(i, n_blk)], sems.at[slot])

    @pl.when(mine)
    def _():
        @pl.loop(0, steps)
        def _(i):
            slot = lax.rem(i, 2)

            @pl.when(i >= 2)
            def _():
                copy(i - 2, slot).wait()

            l = lax.div(i, n_blk)
            at = pl.ds(pl.multiple_of(lax.rem(i, n_blk) * blk, blk), blk)
            for j in range(n_blk):
                buf[slot, j * blk : (j + 1) * blk, :] = w[l, j, at, :].T
            copy(i, slot).start()

        copy(steps - 2, 0).wait()
        copy(steps - 1, 1).wait()


def forward_kernel(tick, info, x_in, inp, w, su_i, sx_i, sd_i, sr_i, y, su, sx, sd, sr):
    del su_i, sx_i, sd_i, sr_i
    n_blk, width, blk = w.shape[1:]
    inv = width ** (-0.5)
    place = info[1]
    chunk = tick - SKEW * place

    @pl.when((chunk >= 0) & (chunk < CHUNKS))
    def _():
        @pl.when(place == 0)
        def _():
            y[...] = inp[chunk]

        @pl.when(place != 0)
        def _():
            y[...] = x_in[...]

        @pl.loop(0, PAIR)
        def _(l):
            xb = y[...]
            x = xb.astype(F32)
            scale = lax.rsqrt(jnp.mean(x * x, axis=-1, keepdims=True) + EPS)
            sx[l, chunk] = xb
            sr[l, chunk] = jnp.broadcast_to(scale, sr.shape[2:])
            su[l, chunk] = (x * scale).astype(BF16)

            @pl.loop(0, 2)
            def _(part):
                for i in range(n_blk // 2):
                    j = part * (n_blk // 2) + i
                    cols = pl.ds(pl.multiple_of(info[2 + j], blk), blk)
                    z = dot(su[l, chunk], w[l, j]) * inv
                    sg = jax.nn.sigmoid(z)
                    sd[l, chunk, :, pl.ds(pl.multiple_of(j * blk, blk), blk)] = sg * (1.0 + z * (1.0 - sg)) * inv
                    y[:, cols] = (sx[l, chunk, :, cols].astype(F32) + z * sg).astype(BF16)


def backward_section(l, chunk, info, w, sx, sd, sr, dx, sq, qrel, du):
    n_blk, _, blk = w.shape[1:]
    for j in range(n_blk):
        cols = pl.ds(pl.multiple_of(info[2 + j], blk), blk)
        q = (dx[:, cols].astype(F32) * sd[l, chunk, :, j * blk : (j + 1) * blk]).astype(BF16)
        qrel[:, j * blk : (j + 1) * blk] = q
        sq[l, chunk, :, cols] = q

    @pl.loop(0, 2)
    def _(part):
        for i in range(n_blk // 2):
            k = part * (n_blk // 2) + i
            du[:, pl.ds(pl.multiple_of(k * blk, blk), blk)] = dot(qrel[...], w[l, k])

    scale = sr[l, chunk][:, :1]
    n = sx[l, chunk].astype(F32) * scale
    g = du[...]
    back = dx[...].astype(F32) + scale * (g - n * jnp.mean(g * n, axis=-1, keepdims=True))
    dx[...] = back.astype(BF16)


def backward_kernel(tick, stages, info, g_in, cot, w, sx, sd, sr, sq_i, dx, sq, qrel, du):
    del sq_i
    place = stages - 1 - info[1]
    chunk = tick - SKEW * place

    @pl.when((chunk >= 0) & (chunk < CHUNKS))
    def _():
        @pl.when(place == 0)
        def _():
            dx[...] = cot[chunk]

        @pl.when(place != 0)
        def _():
            dx[...] = g_in[...]

        @pl.loop(0, PAIR)
        def _(step):
            backward_section(PAIR - 1 - step, chunk, info, w, sx, sd, sr, dx, sq, qrel, du)


def turn_kernel(stages, info, cot, w_in, sx, sd, sr, sq_i, t, dx, sq, w, qrel, du, sems):
    del w_in, sq_i
    half = w.shape[1] // 2
    copies = [
        [
            pltpu.make_async_copy(t.at[l, pl.ds(h * half, half)], w.at[l, pl.ds(h * half, half)], sems.at[l, h])
            for h in range(2)
        ]
        for l in range(PAIR)
    ]
    for l in reversed(range(PAIR)):
        for copy in copies[l]:
            copy.start()
    last = info[1] == stages - 1

    @pl.when(last)
    def _():
        dx[...] = cot[0]

    for l in reversed(range(PAIR)):
        for copy in copies[l]:
            copy.wait()

        @pl.when(last)
        def _():
            backward_section(l, 0, info, w, sx, sd, sr, dx, sq, qrel, du)


def pack_kernel(info, su, sq, out):
    other = 1 - info[0]
    out[0] = su[other]
    out[1] = sq[other]


def gradient_kernel(info, su, sq, recv, out):
    core = info[0]
    depth, width = out.shape
    cols = pl.ds(pl.multiple_of(pl.program_id(0) * depth, depth), depth)
    tokens = lambda v: v.reshape(-1, v.shape[-1])
    u = jnp.concatenate([tokens(su[core, :, :, cols]), tokens(recv[0, :, :, cols])], 0)
    for k in range(0, width, 512):
        q = jnp.concatenate([tokens(sq[core, :, :, k : k + 512]), tokens(recv[1, :, :, k : k + 512])], 0)
        part = lax.dot_general(u, q, (((0,), (0,)), ((), ())), preferred_element_type=F32)
        out[:, k : k + 512] = part.astype(BF16)


VM = pl.BlockSpec(memory_space=pltpu.VMEM)
SM = pl.BlockSpec(memory_space=pltpu.SMEM)
HB = pl.BlockSpec(memory_space=pltpu.HBM)


def cost(flops):
    return pl.CostEstimate(flops=flops, bytes_accessed=0, transcendentals=0)


def params(mib):
    return pltpu.CompilerParams(vmem_limit_bytes=mib * 1024 * 1024)


def body(inputs, cotangent, w_prev, w_now, grads_prev):
    n_dp = lax.axis_size("dp")
    n_sec = lax.axis_size("section")
    stages = n_sec // PAIR
    _, tok_mb, width = inputs.shape
    blk = w_prev.shape[2]
    rows = tok_mb // CHUNKS
    sec = lax.axis_index("section")
    core = sec % PAIR
    stage = sec // PAIR
    dp = lax.axis_index("dp")
    n_y = n_dp // 2

    def over_dp(move):
        pairs = []
        for y in range(n_y):
            for z in range(2):
                ty, tz = move(y, z)
                pairs.append((2 * y + z, 2 * (ty % n_y) + tz))
        return lambda v: lax.ppermute(v, "dp", pairs)

    swap_z = over_dp(lambda y, z: (y, 1 - z))
    to_up = over_dp(lambda y, z: (y + 1, z))
    to_down = over_dp(lambda y, z: (y - 1, z))
    swap_core = lambda v: lax.ppermute(v, "section", [(s, s ^ 1) for s in range(n_sec)])

    lanes = blk // 2
    own = w_prev[0].astype(BF16).reshape(width, 2, lanes).transpose(1, 0, 2)
    pick = lambda v, at: lax.dynamic_index_in_dim(v, at, 0, keepdims=False)
    inp = pick(inputs, core).reshape(CHUNKS, rows, width)
    cot = pick(cotangent, core).reshape(CHUNKS, rows, width)

    def swap_each(*values):
        swapped = []
        for v in values:
            if swapped:
                v, swapped[-1] = lax.optimization_barrier((v, swapped[-1]))
            swapped.append(swap_core(v))
        return swapped

    def linked(*moves):
        return [move(v) for move, v in moves]

    zo, below, above, own_o = lax.optimization_barrier(
        (*linked((swap_z, own), (to_up, own), (to_down, own)), *swap_each(own))
    )
    above, inp, cot = lax.optimization_barrier((above, inp, cot))
    above_z, below_z, far, zo_o, below_o, above_o = lax.optimization_barrier(
        (*linked((swap_z, above), (to_up, zo), (to_down, above)), *swap_each(zo, below, above))
    )
    far_za, far_zb, above_zo, below_zo, far_o = lax.optimization_barrier(
        (*linked((to_up, below_z[:1]), (to_down, above_z[1:])), *swap_each(above_z, below_z, far))
    )
    y_at, z_at = dp // 2, dp % 2
    rel = [(0, 0), (0, 1), (1, 0), (1, 1), (2, 0), (2, 1), (n_y - 1, 0), (n_y - 1, 1)]
    off = [(((y_at + dy) % n_y) * 2 + (z_at + dz) % 2) * blk + h * lanes for dy, dz in rel for h in range(2)]
    info = jnp.stack([core, stage] + off).astype(jnp.int32)
    far_zao, far_zbo, gp, inp, cot, info_late = lax.optimization_barrier(
        (*swap_each(far_za, far_zb), grads_prev, inp, cot, info)
    )
    shares = lax.psum_scatter(gp[0, 0], "dp", scatter_dimension=1, tiled=True)

    saved = (PAIR, CHUNKS, rows, width)
    w_all = pltpu.VMEM((PAIR, 2 * n_dp, width, lanes), BF16)
    in_hbm = lambda *vs: [pltpu.with_memory_space_constraint(v, pltpu.HBM) for v in vs]
    info = info_late
    mine = (own, zo, above, above_z, far, far_za, far_zb, below, below_z)
    other = (own_o, zo_o, above_o, above_zo, far_o, far_zao, far_zbo, below_o, below_zo)
    w_res, su, sx, sd, sr, sq, first = pl.pallas_call(
        assemble_kernel,
        out_shape=[
            w_all,
            pltpu.VMEM(saved, BF16),
            pltpu.VMEM(saved, BF16),
            pltpu.VMEM(saved, F32),
            pltpu.VMEM((PAIR, CHUNKS, rows, 128), F32),
            pltpu.VMEM(saved, BF16),
            pltpu.VMEM((rows, width), BF16),
        ],
        in_specs=[SM] + [HB] * 18,
        out_specs=[VM] * 7,
        scratch_shapes=[pltpu.SemaphoreType.DMA((18,))],
        compiler_params=params(1),
        name="assemble",
    )(info, *in_hbm(*mine, *other))

    def transposed(early, w, *t):
        return pl.pallas_call(
            functools.partial(transpose_kernel, early, stages),
            out_shape=pltpu.HBM(w.shape, w.dtype),
            in_specs=[SM, VM] + [HB] * len(t),
            out_specs=HB,
            input_output_aliases={2: 0} if t else {},
            scratch_shapes=[pltpu.VMEM((2, width, lanes), BF16), pltpu.SemaphoreType.DMA((2,))],
            compiler_params=params(2),
            name="transpose",
        )(info, w, *in_hbm(*t))

    def forward_call(tick, *args):
        return pl.pallas_call(
            functools.partial(forward_kernel, tick),
            out_shape=[
                pltpu.VMEM((rows, width), BF16),
                pltpu.VMEM(su.shape, su.dtype),
                pltpu.VMEM(sx.shape, sx.dtype),
                pltpu.VMEM(sd.shape, sd.dtype),
                pltpu.VMEM(sr.shape, sr.dtype),
            ],
            in_specs=[SM] + [VM] * 7,
            out_specs=[VM] * 5,
            input_output_aliases={4: 1, 5: 2, 6: 3, 7: 4},
            compiler_params=params(1),
            cost_estimate=cost(PAIR * 2 * rows * width * width),
            name="forward",
        )(info, *args)

    def backward_call(tick, *args):
        return pl.pallas_call(
            functools.partial(backward_kernel, tick, stages),
            out_shape=[pltpu.VMEM((rows, width), BF16), pltpu.VMEM(sq.shape, sq.dtype)],
            in_specs=[SM] + [VM] * 7,
            out_specs=[VM] * 2,
            scratch_shapes=[pltpu.VMEM((rows, width), BF16), pltpu.VMEM((rows, width), F32)],
            input_output_aliases={7: 1},
            compiler_params=params(1),
            cost_estimate=cost(PAIR * 2 * rows * width * width),
            name="backward",
        )(info, *args)

    def turn_call(*args):
        return pl.pallas_call(
            functools.partial(turn_kernel, stages),
            out_shape=[pltpu.VMEM((rows, width), BF16), pltpu.VMEM(sq.shape, sq.dtype), w_all],
            in_specs=[SM] + [VM] * 6 + [HB],
            out_specs=[VM] * 3,
            scratch_shapes=[
                pltpu.VMEM((rows, width), BF16),
                pltpu.VMEM((rows, width), F32),
                pltpu.SemaphoreType.DMA((PAIR, 2)),
            ],
            input_output_aliases={6: 1, 2: 2},
            compiler_params=params(1),
            cost_estimate=cost(PAIR * 2 * rows * width * width),
            name="turn",
        )(info, *args)

    ticks = SKEW * (stages - 1) + CHUNKS

    def hop(value, tick, step):
        pairs = []
        for p in range(stages - 1):
            if 0 <= tick - SKEW * p < CHUNKS:
                a, b = (p, p + 1) if step > 0 else (stages - 1 - p, stages - 2 - p)
                pairs += [(PAIR * a + c, PAIR * b + c) for c in range(PAIR)]
        return lax.ppermute(value, "section", pairs) if pairs else None

    def relay(step, call):
        arrived = {}
        for tick in range(ticks):
            arrived[tick] = hop(call(tick, arrived.get(tick - SKEW)), tick, step)

    state = [w_res, su, sx, sd, sr, sq]
    flipped = []

    def forward(tick, arrived):
        if tick in (0, SKEW * (stages // 2) + CHUNKS):
            flipped[:], state[1] = lax.optimization_barrier(([transposed(tick == 0, state[0], *flipped)], state[1]))
        x_in = first if arrived is None else arrived
        y, *state[1:5] = forward_call(tick, x_in, inp, *state[:5])
        return y

    def backward(tick, arrived):
        if tick == 0:
            g, state[5], state[0] = turn_call(cot, state[0], *state[2:6], *in_hbm(flipped[0]))
            return g
        g_in = first if arrived is None else arrived
        g, state[5] = backward_call(tick, g_in, cot, state[0], *state[2:6])
        return g

    relay(1, forward)
    relay(-1, backward)
    su, sq = state[1], state[5]

    packed = pl.pallas_call(
        pack_kernel,
        out_shape=pltpu.VMEM((2,) + saved[1:], BF16),
        in_specs=[SM, VM, VM],
        out_specs=VM,
        compiler_params=params(1),
        name="pack",
    )(info, su, sq)
    dweight = pl.pallas_call(
        gradient_kernel,
        grid=(width // 256,),
        out_shape=jax.ShapeDtypeStruct((width, width), BF16),
        in_specs=[SM] + [VM] * 3,
        out_specs=pl.BlockSpec((256, width), lambda i: (i, 0)),
        compiler_params=params(8),
        cost_estimate=cost(4 * tok_mb * width * width),
        name="gradient",
    )(info, su, sq, swap_core(packed))
    grads_next = dweight[None, None]
    w_next = w_now - LEARN_RATE / n_dp * shares.astype(F32)[None]
    return (w_next, grads_next)


def solution(mesh):
    placed = (
        P(None, "dp", None),
        P(None, "dp", None),
        P("section", None, "dp"),
        P("section", None, "dp"),
        P("dp", "section", None, None),
    )
    return jax.shard_map(
        body,
        mesh=mesh,
        in_specs=placed,
        out_specs=(P("section", None, "dp"), P("dp", "section", None, None)),
        check_vma=False,
    )
```

```python
import functools

import jax
import jax.numpy as jnp
from jax import lax
from jax.experimental import pallas as pl
from jax.experimental.pallas import tpu as pltpu
from jax.sharding import PartitionSpec as P


EPS = 1e-06
LEARN_RATE = 1.0
CHUNKS = 4
SKEW = 2
PAIR = 2
F32 = jnp.float32
BF16 = jnp.bfloat16


def dot(a, b):
    return jnp.dot(a, b, preferred_element_type=F32)


def transpose_kernel(early, stages, info, w, *refs):
    t, buf, sems = refs[-3:]
    n_blk, _, blk = w.shape[1:]
    mine = info[1] * 2 >= stages if early else info[1] * 2 < stages
    steps = PAIR * n_blk

    def copy(i, slot):
        return pltpu.make_async_copy(buf.at[slot], t.at[lax.div(i, n_blk), lax.rem(i, n_blk)], sems.at[slot])

    @pl.when(mine)
    def _():
        @pl.loop(0, steps)
        def _(i):
            slot = lax.rem(i, 2)

            @pl.when(i >= 2)
            def _():
                copy(i - 2, slot).wait()

            l = lax.div(i, n_blk)
            at = pl.ds(pl.multiple_of(lax.rem(i, n_blk) * blk, blk), blk)
            for j in range(n_blk):
                buf[slot, j * blk : (j + 1) * blk, :] = w[l, j, at, :].T
            copy(i, slot).start()

        copy(steps - 2, 0).wait()
        copy(steps - 1, 1).wait()


def forward_section(l, chunk, info, w, y, su, sx, sd, sr):
    n_blk, width, blk = w.shape[1:]
    inv = width ** (-0.5)
    xb = y[...]
    x = xb.astype(F32)
    scale = lax.rsqrt(jnp.mean(x * x, axis=-1, keepdims=True) + EPS)
    sx[l, chunk] = xb
    sr[l, chunk] = jnp.broadcast_to(scale, sr.shape[2:])
    su[l, chunk] = (x * scale).astype(BF16)

    @pl.loop(0, 2)
    def _(part):
        for i in range(n_blk // 2):
            j = part * (n_blk // 2) + i
            cols = pl.ds(pl.multiple_of(info[2 + j], blk), blk)
            z = dot(su[l, chunk], w[l, j]) * inv
            sg = jax.nn.sigmoid(z)
            sd[l, chunk, :, pl.ds(pl.multiple_of(j * blk, blk), blk)] = sg * (1.0 + z * (1.0 - sg)) * inv
            y[:, cols] = (sx[l, chunk, :, cols].astype(F32) + z * sg).astype(BF16)


def forward_kernel(tick, info, x_in, inp, w, su_i, sx_i, sd_i, sr_i, y, su, sx, sd, sr):
    del su_i, sx_i, sd_i, sr_i
    place = info[1]
    chunk = tick - SKEW * place

    @pl.when((chunk >= 0) & (chunk < CHUNKS))
    def _():
        @pl.when(place == 0)
        def _():
            y[...] = inp[chunk]

        @pl.when(place != 0)
        def _():
            y[...] = x_in[...]

        @pl.loop(0, PAIR)
        def _(l):
            forward_section(l, chunk, info, w, y, su, sx, sd, sr)


def start_kernel(info, inp, *refs):
    mine, other = refs[:9], refs[9:18]
    y, w, su, sx, sd, sr, sq, first, sems = refs[18:]
    del sq, first
    core = info[0]
    active = info[1] == 0

    def copies(slot, blocks):
        for i, (at, block) in enumerate(zip((0, 2, 4, 6, 8, 10, 11, 12, 14), blocks)):
            yield pltpu.make_async_copy(block, w.at[slot, pl.ds(at, block.shape[0])], sems.at[slot, i])

    def start(slot):
        for here, blocks in ((core == slot, mine), (core != slot, other)):

            @pl.when(here)
            def _():
                for copy in copies(slot, blocks):
                    copy.start()

    @pl.when(active)
    def _():
        y[...] = inp[0]

    start(0)
    for l in range(PAIR):
        for copy in copies(l, mine):
            copy.wait()
        if l + 1 < PAIR:
            start(l + 1)

        @pl.when(active)
        def _():
            forward_section(l, 0, info, w, y, su, sx, sd, sr)


def backward_section(l, chunk, info, w, sx, sd, sr, dx, sq, qrel, du):
    n_blk, _, blk = w.shape[1:]
    for j in range(n_blk):
        cols = pl.ds(pl.multiple_of(info[2 + j], blk), blk)
        q = (dx[:, cols].astype(F32) * sd[l, chunk, :, j * blk : (j + 1) * blk]).astype(BF16)
        qrel[:, j * blk : (j + 1) * blk] = q
        sq[l, chunk, :, cols] = q

    @pl.loop(0, 2)
    def _(part):
        for i in range(n_blk // 2):
            k = part * (n_blk // 2) + i
            du[:, pl.ds(pl.multiple_of(k * blk, blk), blk)] = dot(qrel[...], w[l, k])

    scale = sr[l, chunk][:, :1]
    n = sx[l, chunk].astype(F32) * scale
    g = du[...]
    back = dx[...].astype(F32) + scale * (g - n * jnp.mean(g * n, axis=-1, keepdims=True))
    dx[...] = back.astype(BF16)


def backward_kernel(tick, stages, info, g_in, cot, w, sx, sd, sr, sq_i, dx, sq, qrel, du):
    del sq_i
    place = stages - 1 - info[1]
    chunk = tick - SKEW * place

    @pl.when((chunk >= 0) & (chunk < CHUNKS))
    def _():
        @pl.when(place == 0)
        def _():
            dx[...] = cot[chunk]

        @pl.when(place != 0)
        def _():
            dx[...] = g_in[...]

        @pl.loop(0, PAIR)
        def _(step):
            backward_section(PAIR - 1 - step, chunk, info, w, sx, sd, sr, dx, sq, qrel, du)


def turn_kernel(stages, info, cot, w_in, sx, sd, sr, sq_i, t, dx, sq, w, qrel, du, sems):
    del w_in, sq_i
    half = w.shape[1] // 2
    copies = [
        [
            pltpu.make_async_copy(t.at[l, pl.ds(h * half, half)], w.at[l, pl.ds(h * half, half)], sems.at[l, h])
            for h in range(2)
        ]
        for l in range(PAIR)
    ]
    for copy in copies[PAIR - 1]:
        copy.start()
    last = info[1] == stages - 1

    @pl.when(last)
    def _():
        dx[...] = cot[0]

    for l in reversed(range(PAIR)):
        for copy in copies[l]:
            copy.wait()
        if l > 0:
            for copy in copies[l - 1]:
                copy.start()

        @pl.when(last)
        def _():
            backward_section(l, 0, info, w, sx, sd, sr, dx, sq, qrel, du)


def pack_kernel(info, su, sq, out):
    other = 1 - info[0]
    out[0] = su[other]
    out[1] = sq[other]


def gradient_kernel(share, info, su, sq, recv, w_now, total, out, w_next):
    core = info[0]
    depth, width = out.shape
    cols = pl.ds(pl.multiple_of(pl.program_id(0) * depth, depth), depth)
    tokens = lambda v: v.reshape(-1, v.shape[-1])
    u = jnp.concatenate([tokens(su[core, :, :, cols]), tokens(recv[0, :, :, cols])], 0).T
    for k in range(0, width, 512):
        q = jnp.concatenate([tokens(sq[core, :, :, k : k + 512]), tokens(recv[1, :, :, k : k + 512])], 0)
        out[:, k : k + 512] = dot(u, q).astype(BF16)
    w_next[...] = w_now[...] - share * total[...].astype(F32)


VM = pl.BlockSpec(memory_space=pltpu.VMEM)
SM = pl.BlockSpec(memory_space=pltpu.SMEM)
HB = pl.BlockSpec(memory_space=pltpu.HBM)


def cost(flops):
    return pl.CostEstimate(flops=flops, bytes_accessed=0, transcendentals=0)


def params(mib):
    return pltpu.CompilerParams(vmem_limit_bytes=mib * 1024 * 1024)


def body(inputs, cotangent, w_prev, w_now, grads_prev):
    n_dp = lax.axis_size("dp")
    n_sec = lax.axis_size("section")
    stages = n_sec // PAIR
    _, tok_mb, width = inputs.shape
    blk = w_prev.shape[2]
    rows = tok_mb // CHUNKS
    sec = lax.axis_index("section")
    core = sec % PAIR
    stage = sec // PAIR
    dp = lax.axis_index("dp")
    n_y = n_dp // 2

    def over_dp(move):
        pairs = []
        for y in range(n_y):
            for z in range(2):
                ty, tz = move(y, z)
                pairs.append((2 * y + z, 2 * (ty % n_y) + tz))
        return lambda v: lax.ppermute(v, "dp", pairs)

    swap_z = over_dp(lambda y, z: (y, 1 - z))
    to_up = over_dp(lambda y, z: (y + 1, z))
    to_down = over_dp(lambda y, z: (y - 1, z))
    swap_core = lambda v: lax.ppermute(v, "section", [(s, s ^ 1) for s in range(n_sec)])

    lanes = blk // 2
    own = w_prev[0].astype(BF16).reshape(width, 2, lanes).transpose(1, 0, 2)
    pick = lambda v, at: lax.dynamic_index_in_dim(v, at, 0, keepdims=False)
    inp = pick(inputs, core).reshape(CHUNKS, rows, width)
    cot = pick(cotangent, core).reshape(CHUNKS, rows, width)

    def swap_each(*values):
        swapped = []
        for v in values:
            if swapped:
                v, swapped[-1] = lax.optimization_barrier((v, swapped[-1]))
            swapped.append(swap_core(v))
        return swapped

    def linked(*moves):
        return [move(v) for move, v in moves]

    zo, below, above, own_o = lax.optimization_barrier(
        (*linked((swap_z, own), (to_up, own), (to_down, own)), *swap_each(own))
    )
    above, inp, cot = lax.optimization_barrier((above, inp, cot))
    above_z, below_z, far, zo_o, below_o, above_o = lax.optimization_barrier(
        (*linked((swap_z, above), (to_up, zo), (to_down, above)), *swap_each(zo, below, above))
    )
    far_za, far_zb, above_zo, below_zo, far_o = lax.optimization_barrier(
        (*linked((to_up, below_z[:1]), (to_down, above_z[1:])), *swap_each(above_z, below_z, far))
    )
    y_at, z_at = dp // 2, dp % 2
    rel = [(0, 0), (0, 1), (1, 0), (1, 1), (2, 0), (2, 1), (n_y - 1, 0), (n_y - 1, 1)]
    off = [(((y_at + dy) % n_y) * 2 + (z_at + dz) % 2) * blk + h * lanes for dy, dz in rel for h in range(2)]
    info = jnp.stack([core, stage] + off).astype(jnp.int32)
    far_zao, far_zbo, gp, inp, cot, info_late = lax.optimization_barrier(
        (*swap_each(far_za, far_zb), grads_prev, inp, cot, info)
    )
    shares = lax.psum_scatter(gp[0, 0], "dp", scatter_dimension=1, tiled=True)

    saved = (PAIR, CHUNKS, rows, width)
    w_all = pltpu.VMEM((PAIR, 2 * n_dp, width, lanes), BF16)
    in_hbm = lambda *vs: [pltpu.with_memory_space_constraint(v, pltpu.HBM) for v in vs]
    info = info_late
    mine = (own, zo, above, above_z, far, far_za, far_zb, below, below_z)
    other = (own_o, zo_o, above_o, above_zo, far_o, far_zao, far_zbo, below_o, below_zo)
    y_start, w_res, su, sx, sd, sr, sq, first = pl.pallas_call(
        start_kernel,
        out_shape=[
            pltpu.VMEM((rows, width), BF16),
            w_all,
            pltpu.VMEM(saved, BF16),
            pltpu.VMEM(saved, BF16),
            pltpu.VMEM(saved, F32),
            pltpu.VMEM((PAIR, CHUNKS, rows, 128), F32),
            pltpu.VMEM(saved, BF16),
            pltpu.VMEM((rows, width), BF16),
        ],
        in_specs=[SM, VM] + [HB] * 18,
        out_specs=[VM] * 8,
        scratch_shapes=[pltpu.SemaphoreType.DMA((PAIR, 9))],
        compiler_params=params(1),
        cost_estimate=cost(PAIR * 2 * rows * width * width),
        name="start",
    )(info, inp, *in_hbm(*mine, *other))

    def transposed(early, w, *t):
        return pl.pallas_call(
            functools.partial(transpose_kernel, early, stages),
            out_shape=pltpu.HBM(w.shape, w.dtype),
            in_specs=[SM, VM] + [HB] * len(t),
            out_specs=HB,
            input_output_aliases={2: 0} if t else {},
            scratch_shapes=[pltpu.VMEM((2, width, lanes), BF16), pltpu.SemaphoreType.DMA((2,))],
            compiler_params=params(2),
            name="transpose",
        )(info, w, *in_hbm(*t))

    def forward_call(tick, *args):
        return pl.pallas_call(
            functools.partial(forward_kernel, tick),
            out_shape=[
                pltpu.VMEM((rows, width), BF16),
                pltpu.VMEM(su.shape, su.dtype),
                pltpu.VMEM(sx.shape, sx.dtype),
                pltpu.VMEM(sd.shape, sd.dtype),
                pltpu.VMEM(sr.shape, sr.dtype),
            ],
            in_specs=[SM] + [VM] * 7,
            out_specs=[VM] * 5,
            input_output_aliases={4: 1, 5: 2, 6: 3, 7: 4},
            compiler_params=params(1),
            cost_estimate=cost(PAIR * 2 * rows * width * width),
            name="forward",
        )(info, *args)

    def backward_call(tick, *args):
        return pl.pallas_call(
            functools.partial(backward_kernel, tick, stages),
            out_shape=[pltpu.VMEM((rows, width), BF16), pltpu.VMEM(sq.shape, sq.dtype)],
            in_specs=[SM] + [VM] * 7,
            out_specs=[VM] * 2,
            scratch_shapes=[pltpu.VMEM((rows, width), BF16), pltpu.VMEM((rows, width), F32)],
            input_output_aliases={7: 1},
            compiler_params=params(1),
            cost_estimate=cost(PAIR * 2 * rows * width * width),
            name="backward",
        )(info, *args)

    def turn_call(*args):
        return pl.pallas_call(
            functools.partial(turn_kernel, stages),
            out_shape=[pltpu.VMEM((rows, width), BF16), pltpu.VMEM(sq.shape, sq.dtype), w_all],
            in_specs=[SM] + [VM] * 6 + [HB],
            out_specs=[VM] * 3,
            scratch_shapes=[
                pltpu.VMEM((rows, width), BF16),
                pltpu.VMEM((rows, width), F32),
                pltpu.SemaphoreType.DMA((PAIR, 2)),
            ],
            input_output_aliases={6: 1, 2: 2},
            compiler_params=params(1),
            cost_estimate=cost(PAIR * 2 * rows * width * width),
            name="turn",
        )(info, *args)

    ticks = SKEW * (stages - 1) + CHUNKS

    def hop(value, tick, step):
        pairs = []
        for p in range(stages - 1):
            if 0 <= tick - SKEW * p < CHUNKS:
                a, b = (p, p + 1) if step > 0 else (stages - 1 - p, stages - 2 - p)
                pairs += [(PAIR * a + c, PAIR * b + c) for c in range(PAIR)]
        return lax.ppermute(value, "section", pairs) if pairs else None

    def relay(step, call):
        arrived = {}
        for tick in range(ticks):
            arrived[tick] = hop(call(tick, arrived.get(tick - SKEW)), tick, step)

    state = [w_res, su, sx, sd, sr, sq]
    flipped = []

    def forward(tick, arrived):
        if tick == 0:
            return y_start
        if tick in (1, SKEW * (stages // 2) + CHUNKS):
            flipped[:], state[1] = lax.optimization_barrier(([transposed(tick == 1, state[0], *flipped)], state[1]))
        x_in = first if arrived is None else arrived
        y, *state[1:5] = forward_call(tick, x_in, inp, *state[:5])
        return y

    def backward(tick, arrived):
        if tick == 0:
            g, state[5], state[0] = turn_call(cot, state[0], *state[2:6], *in_hbm(flipped[0]))
            return g
        g_in = first if arrived is None else arrived
        g, state[5] = backward_call(tick, g_in, cot, state[0], *state[2:6])
        return g

    relay(1, forward)
    relay(-1, backward)
    su, sq = state[1], state[5]

    packed = pl.pallas_call(
        pack_kernel,
        out_shape=pltpu.VMEM((2,) + saved[1:], BF16),
        in_specs=[SM, VM, VM],
        out_specs=VM,
        compiler_params=params(1),
        name="pack",
    )(info, su, sq)
    depth = 512
    row_block = lambda cols: pl.BlockSpec((depth, cols), lambda i: (i, 0))
    dweight, w_next = pl.pallas_call(
        functools.partial(gradient_kernel, LEARN_RATE / n_dp),
        grid=(width // depth,),
        out_shape=[jax.ShapeDtypeStruct((width, width), BF16), jax.ShapeDtypeStruct((width, blk), F32)],
        in_specs=[SM] + [VM] * 3 + [row_block(blk)] * 2,
        out_specs=[row_block(width), row_block(blk)],
        compiler_params=params(12),
        cost_estimate=cost(4 * tok_mb * width * width),
        name="gradient",
    )(info, su, sq, swap_core(packed), *in_hbm(w_now[0], shares))
    return (w_next[None], dweight[None, None])


def solution(mesh):
    placed = (
        P(None, "dp", None),
        P(None, "dp", None),
        P("section", None, "dp"),
        P("section", None, "dp"),
        P("dp", "section", None, None),
    )
    return jax.shard_map(
        body,
        mesh=mesh,
        in_specs=placed,
        out_specs=(P("section", None, "dp"), P("dp", "section", None, None)),
        check_vma=False,
    )
```

```python
import functools

import jax
import jax.numpy as jnp
from jax import lax
from jax.experimental import pallas as pl
from jax.experimental.pallas import tpu as pltpu
from jax.sharding import PartitionSpec as P


EPS = 1e-06
LEARN_RATE = 1.0
CHUNKS = 4
SKEW = 2
PAIR = 2
F32 = jnp.float32
BF16 = jnp.bfloat16


def dot(a, b):
    return jnp.dot(a, b, preferred_element_type=F32)


def transpose_kernel(early, stages, info, w, *refs):
    t, buf, sems = refs[-3:]
    n_blk, _, blk = w.shape[1:]
    mine = info[1] * 2 >= stages if early else info[1] * 2 < stages
    steps = PAIR * n_blk

    def copy(i, slot):
        return pltpu.make_async_copy(buf.at[slot], t.at[lax.div(i, n_blk), lax.rem(i, n_blk)], sems.at[slot])

    @pl.when(mine)
    def _():
        @pl.loop(0, steps)
        def _(i):
            slot = lax.rem(i, 2)

            @pl.when(i >= 2)
            def _():
                copy(i - 2, slot).wait()

            l = lax.div(i, n_blk)
            at = pl.ds(pl.multiple_of(lax.rem(i, n_blk) * blk, blk), blk)
            for j in range(n_blk):
                buf[slot, j * blk : (j + 1) * blk, :] = w[l, j, at, :].T
            copy(i, slot).start()

        copy(steps - 2, 0).wait()
        copy(steps - 1, 1).wait()


def forward_section(l, chunk, info, w, y, su, sx, sd, sr):
    n_blk, width, blk = w.shape[1:]
    inv = width ** (-0.5)
    xb = y[...]
    x = xb.astype(F32)
    scale = lax.rsqrt(jnp.mean(x * x, axis=-1, keepdims=True) + EPS)
    sx[l, chunk] = xb
    sr[l, chunk] = jnp.broadcast_to(scale, sr.shape[2:])
    su[l, chunk] = (x * scale).astype(BF16)

    @pl.loop(0, 2)
    def _(part):
        for i in range(n_blk // 2):
            j = part * (n_blk // 2) + i
            cols = pl.ds(pl.multiple_of(info[2 + j], blk), blk)
            z = dot(su[l, chunk], w[l, j]) * inv
            sg = jax.nn.sigmoid(z)
            sd[l, chunk, :, pl.ds(pl.multiple_of(j * blk, blk), blk)] = sg * (1.0 + z * (1.0 - sg)) * inv
            y[:, cols] = (sx[l, chunk, :, cols].astype(F32) + z * sg).astype(BF16)


def forward_kernel(tick, info, x_in, inp, w, su_i, sx_i, sd_i, sr_i, y, su, sx, sd, sr):
    del su_i, sx_i, sd_i, sr_i
    place = info[1]
    chunk = tick - SKEW * place

    @pl.when((chunk >= 0) & (chunk < CHUNKS))
    def _():
        @pl.when(place == 0)
        def _():
            y[...] = inp[chunk]

        @pl.when(place != 0)
        def _():
            y[...] = x_in[...]

        @pl.loop(0, PAIR)
        def _(l):
            forward_section(l, chunk, info, w, y, su, sx, sd, sr)


def start_kernel(info, inp, *refs):
    mine, other = refs[:8], refs[8:16]
    y, w, su, sx, sd, sr, sq, first, sems = refs[16:]
    del sq, first
    core = info[0]
    active = info[1] == 0

    def copies(slot, blocks):
        for i, block in enumerate(blocks):
            yield pltpu.make_async_copy(block, w.at[slot, pl.ds(2 * i, 2)], sems.at[slot, i])

    def start(slot):
        for here, blocks in ((core == slot, mine), (core != slot, other)):

            @pl.when(here)
            def _():
                for copy in copies(slot, blocks):
                    copy.start()

    @pl.when(active)
    def _():
        y[...] = inp[0]

    for slot in range(PAIR):
        start(slot)

    @pl.loop(0, PAIR)
    def _(l):
        for copy in copies(l, mine):
            copy.wait()

        @pl.when(active)
        def _():
            forward_section(l, 0, info, w, y, su, sx, sd, sr)


def backward_section(l, chunk, info, w, sx, sd, sr, dx, sq, qrel, du):
    n_blk, _, blk = w.shape[1:]
    for j in range(n_blk):
        cols = pl.ds(pl.multiple_of(info[2 + j], blk), blk)
        q = (dx[:, cols].astype(F32) * sd[l, chunk, :, j * blk : (j + 1) * blk]).astype(BF16)
        qrel[:, j * blk : (j + 1) * blk] = q
        sq[l, chunk, :, cols] = q

    @pl.loop(0, 2)
    def _(part):
        for i in range(n_blk // 2):
            k = part * (n_blk // 2) + i
            du[:, pl.ds(pl.multiple_of(k * blk, blk), blk)] = dot(qrel[...], w[l, k])

    scale = sr[l, chunk][:, :1]
    n = sx[l, chunk].astype(F32) * scale
    g = du[...]
    back = dx[...].astype(F32) + scale * (g - n * jnp.mean(g * n, axis=-1, keepdims=True))
    dx[...] = back.astype(BF16)


def backward_kernel(tick, stages, info, g_in, cot, w, sx, sd, sr, sq_i, dx, sq, qrel, du):
    del sq_i
    place = stages - 1 - info[1]
    chunk = tick - SKEW * place

    @pl.when((chunk >= 0) & (chunk < CHUNKS))
    def _():
        @pl.when(place == 0)
        def _():
            dx[...] = cot[chunk]

        @pl.when(place != 0)
        def _():
            dx[...] = g_in[...]

        @pl.loop(0, PAIR)
        def _(step):
            backward_section(PAIR - 1 - step, chunk, info, w, sx, sd, sr, dx, sq, qrel, du)


def turn_kernel(stages, info, cot, w_in, sx, sd, sr, sq_i, t, dx, sq, w, qrel, du, sems):
    del w_in, sq_i
    half = w.shape[1] // 2

    def copies(l):
        for h in range(2):
            at = pl.ds(h * half, half)
            yield pltpu.make_async_copy(t.at[l, at], w.at[l, at], sems.at[l, h])

    for l in reversed(range(PAIR)):
        for copy in copies(l):
            copy.start()
    last = info[1] == stages - 1

    @pl.when(last)
    def _():
        dx[...] = cot[0]

    @pl.loop(0, PAIR)
    def _(step):
        l = PAIR - 1 - step
        for copy in copies(l):
            copy.wait()

        @pl.when(last)
        def _():
            backward_section(l, 0, info, w, sx, sd, sr, dx, sq, qrel, du)


def pack_kernel(info, su, sq, out):
    other = 1 - info[0]
    out[0] = su[other]
    out[1] = sq[other]


def gradient_kernel(share, info, su, sq, recv, w_now, total, out, w_next):
    core = info[0]
    depth, width = out.shape
    cols = pl.ds(pl.multiple_of(pl.program_id(0) * depth, depth), depth)
    tokens = lambda v: v.reshape(-1, v.shape[-1])
    u = jnp.concatenate([tokens(su[core, :, :, cols]), tokens(recv[0, :, :, cols])], 0).T
    for k in range(0, width, 512):
        q = jnp.concatenate([tokens(sq[core, :, :, k : k + 512]), tokens(recv[1, :, :, k : k + 512])], 0)
        out[:, k : k + 512] = dot(u, q).astype(BF16)
    w_next[...] = w_now[...] - share * total[...].astype(F32)


VM = pl.BlockSpec(memory_space=pltpu.VMEM)
SM = pl.BlockSpec(memory_space=pltpu.SMEM)
HB = pl.BlockSpec(memory_space=pltpu.HBM)


def cost(flops):
    return pl.CostEstimate(flops=flops, bytes_accessed=0, transcendentals=0)


def params(mib):
    return pltpu.CompilerParams(vmem_limit_bytes=mib * 1024 * 1024)


def body(inputs, cotangent, w_prev, w_now, grads_prev):
    n_dp = lax.axis_size("dp")
    n_sec = lax.axis_size("section")
    stages = n_sec // PAIR
    _, tok_mb, width = inputs.shape
    blk = w_prev.shape[2]
    rows = tok_mb // CHUNKS
    sec = lax.axis_index("section")
    core = sec % PAIR
    stage = sec // PAIR
    dp = lax.axis_index("dp")
    n_y = n_dp // 2

    def over_dp(move):
        pairs = []
        for y in range(n_y):
            for z in range(2):
                ty, tz = move(y, z)
                pairs.append((2 * y + z, 2 * (ty % n_y) + tz))
        return lambda v: lax.ppermute(v, "dp", pairs)

    swap_z = over_dp(lambda y, z: (y, 1 - z))
    to_up = over_dp(lambda y, z: (y + 1, z))
    to_down = over_dp(lambda y, z: (y - 1, z))
    swap_core = lambda v: lax.ppermute(v, "section", [(s, s ^ 1) for s in range(n_sec)])

    lanes = blk // 2
    own = w_prev[0].astype(BF16).reshape(width, 2, lanes).transpose(1, 0, 2)
    pick = lambda v, at: lax.dynamic_index_in_dim(v, at, 0, keepdims=False)
    inp = pick(inputs, core).reshape(CHUNKS, rows, width)
    cot = pick(cotangent, core).reshape(CHUNKS, rows, width)

    def swap_each(*values):
        swapped = []
        for v in values:
            if swapped:
                v, swapped[-1] = lax.optimization_barrier((v, swapped[-1]))
            swapped.append(swap_core(v))
        return swapped

    def linked(*moves):
        return [move(v) for move, v in moves]

    zo, below, above, own_o = lax.optimization_barrier(
        (*linked((swap_z, own), (to_up, own), (to_down, own)), *swap_each(own))
    )
    above, inp, cot = lax.optimization_barrier((above, inp, cot))
    above_z, below_z, far, zo_o, below_o, above_o = lax.optimization_barrier(
        (*linked((swap_z, above), (to_up, zo), (to_down, above)), *swap_each(zo, below, above))
    )
    far_za, far_zb, above_zo, below_zo, far_o = lax.optimization_barrier(
        (*linked((to_up, below_z[:1]), (to_down, above_z[1:])), *swap_each(above_z, below_z, far))
    )
    y_at, z_at = dp // 2, dp % 2
    rel = [(0, 0), (0, 1), (1, 0), (1, 1), (2, 0), (2, 1), (n_y - 1, 0), (n_y - 1, 1)]
    off = [(((y_at + dy) % n_y) * 2 + (z_at + dz) % 2) * blk + h * lanes for dy, dz in rel for h in range(2)]
    info = jnp.stack([core, stage] + off).astype(jnp.int32)
    far_z = jnp.concatenate([far_za, far_zb], 0)
    far_zo, gp, inp, cot, info_late = lax.optimization_barrier((swap_core(far_z), grads_prev, inp, cot, info))
    shares = lax.psum_scatter(gp[0, 0], "dp", scatter_dimension=1, tiled=True)

    saved = (PAIR, CHUNKS, rows, width)
    w_all = pltpu.VMEM((PAIR, 2 * n_dp, width, lanes), BF16)
    in_hbm = lambda *vs: [pltpu.with_memory_space_constraint(v, pltpu.HBM) for v in vs]
    info = info_late
    mine = (own, zo, above, above_z, far, far_z, below, below_z)
    other = (own_o, zo_o, above_o, above_zo, far_o, far_zo, below_o, below_zo)
    y_start, w_res, su, sx, sd, sr, sq, first = pl.pallas_call(
        start_kernel,
        out_shape=[
            pltpu.VMEM((rows, width), BF16),
            w_all,
            pltpu.VMEM(saved, BF16),
            pltpu.VMEM(saved, BF16),
            pltpu.VMEM(saved, F32),
            pltpu.VMEM((PAIR, CHUNKS, rows, 128), F32),
            pltpu.VMEM(saved, BF16),
            pltpu.VMEM((rows, width), BF16),
        ],
        in_specs=[SM, VM] + [HB] * 16,
        out_specs=[VM] * 8,
        scratch_shapes=[pltpu.SemaphoreType.DMA((PAIR, 8))],
        compiler_params=params(1),
        cost_estimate=cost(PAIR * 2 * rows * width * width),
        name="start",
    )(info, inp, *in_hbm(*mine, *other))

    def transposed(early, w, *t):
        return pl.pallas_call(
            functools.partial(transpose_kernel, early, stages),
            out_shape=pltpu.HBM(w.shape, w.dtype),
            in_specs=[SM, VM] + [HB] * len(t),
            out_specs=HB,
            input_output_aliases={2: 0} if t else {},
            scratch_shapes=[pltpu.VMEM((2, width, lanes), BF16), pltpu.SemaphoreType.DMA((2,))],
            compiler_params=params(2),
            name="transpose",
        )(info, w, *in_hbm(*t))

    def forward_call(tick, *args):
        return pl.pallas_call(
            functools.partial(forward_kernel, tick),
            out_shape=[
                pltpu.VMEM((rows, width), BF16),
                pltpu.VMEM(su.shape, su.dtype),
                pltpu.VMEM(sx.shape, sx.dtype),
                pltpu.VMEM(sd.shape, sd.dtype),
                pltpu.VMEM(sr.shape, sr.dtype),
            ],
            in_specs=[SM] + [VM] * 7,
            out_specs=[VM] * 5,
            input_output_aliases={4: 1, 5: 2, 6: 3, 7: 4},
            compiler_params=params(1),
            cost_estimate=cost(PAIR * 2 * rows * width * width),
            name="forward",
        )(info, *args)

    def backward_call(tick, *args):
        return pl.pallas_call(
            functools.partial(backward_kernel, tick, stages),
            out_shape=[pltpu.VMEM((rows, width), BF16), pltpu.VMEM(sq.shape, sq.dtype)],
            in_specs=[SM] + [VM] * 7,
            out_specs=[VM] * 2,
            scratch_shapes=[pltpu.VMEM((rows, width), BF16), pltpu.VMEM((rows, width), F32)],
            input_output_aliases={7: 1},
            compiler_params=params(1),
            cost_estimate=cost(PAIR * 2 * rows * width * width),
            name="backward",
        )(info, *args)

    def turn_call(*args):
        return pl.pallas_call(
            functools.partial(turn_kernel, stages),
            out_shape=[pltpu.VMEM((rows, width), BF16), pltpu.VMEM(sq.shape, sq.dtype), w_all],
            in_specs=[SM] + [VM] * 6 + [HB],
            out_specs=[VM] * 3,
            scratch_shapes=[
                pltpu.VMEM((rows, width), BF16),
                pltpu.VMEM((rows, width), F32),
                pltpu.SemaphoreType.DMA((PAIR, 2)),
            ],
            input_output_aliases={6: 1, 2: 2},
            compiler_params=params(1),
            cost_estimate=cost(PAIR * 2 * rows * width * width),
            name="turn",
        )(info, *args)

    ticks = SKEW * (stages - 1) + CHUNKS

    def hop(value, tick, step):
        pairs = []
        for p in range(stages - 1):
            if 0 <= tick - SKEW * p < CHUNKS:
                a, b = (p, p + 1) if step > 0 else (stages - 1 - p, stages - 2 - p)
                pairs += [(PAIR * a + c, PAIR * b + c) for c in range(PAIR)]
        return lax.ppermute(value, "section", pairs) if pairs else None

    def relay(step, call):
        arrived = {}
        for tick in range(ticks):
            arrived[tick] = hop(call(tick, arrived.get(tick - SKEW)), tick, step)

    state = [w_res, su, sx, sd, sr, sq]
    flipped = []

    def forward(tick, arrived):
        if tick == 0:
            return y_start
        if tick in (1, SKEW * (stages // 2) + CHUNKS):
            flipped[:], state[1] = lax.optimization_barrier(([transposed(tick == 1, state[0], *flipped)], state[1]))
        x_in = first if arrived is None else arrived
        y, *state[1:5] = forward_call(tick, x_in, inp, *state[:5])
        return y

    def backward(tick, arrived):
        if tick == 0:
            g, state[5], state[0] = turn_call(cot, state[0], *state[2:6], *in_hbm(flipped[0]))
            return g
        g_in = first if arrived is None else arrived
        g, state[5] = backward_call(tick, g_in, cot, state[0], *state[2:6])
        return g

    relay(1, forward)
    relay(-1, backward)
    su, sq = state[1], state[5]

    packed = pl.pallas_call(
        pack_kernel,
        out_shape=pltpu.VMEM((2,) + saved[1:], BF16),
        in_specs=[SM, VM, VM],
        out_specs=VM,
        compiler_params=params(1),
        name="pack",
    )(info, su, sq)
    depth = 512
    row_block = lambda cols: pl.BlockSpec((depth, cols), lambda i: (i, 0))
    dweight, w_next = pl.pallas_call(
        functools.partial(gradient_kernel, LEARN_RATE / n_dp),
        grid=(width // depth,),
        out_shape=[jax.ShapeDtypeStruct((width, width), BF16), jax.ShapeDtypeStruct((width, blk), F32)],
        in_specs=[SM] + [VM] * 3 + [row_block(blk)] * 2,
        out_specs=[row_block(width), row_block(blk)],
        compiler_params=params(12),
        cost_estimate=cost(4 * tok_mb * width * width),
        name="gradient",
    )(info, su, sq, swap_core(packed), *in_hbm(w_now[0], shares))
    return (w_next[None], dweight[None, None])


def solution(mesh):
    placed = (
        P(None, "dp", None),
        P(None, "dp", None),
        P("section", None, "dp"),
        P("section", None, "dp"),
        P("dp", "section", None, None),
    )
    return jax.shard_map(
        body,
        mesh=mesh,
        in_specs=placed,
        out_specs=(P("section", None, "dp"), P("dp", "section", None, None)),
        check_vma=False,
    )
```

```python
import functools

import jax
import jax.numpy as jnp
from jax import lax
from jax.experimental import pallas as pl
from jax.experimental.pallas import tpu as pltpu
from jax.sharding import PartitionSpec as P


EPS = 1e-06
LEARN_RATE = 1.0
CHUNKS = 4
SKEW = 2
PAIR = 2
F32 = jnp.float32
BF16 = jnp.bfloat16


def dot(a, b):
    return jnp.dot(a, b, preferred_element_type=F32)


def round_kernel(w, out):
    lanes = out.shape[2]
    for h in range(2):
        out[h] = w[:, h * lanes : (h + 1) * lanes].astype(BF16)


def transpose_kernel(early, stages, info, w, *refs):
    t, buf, sems = refs[-3:]
    n_blk, _, blk = w.shape[1:]
    mine = info[1] * 2 >= stages if early else info[1] * 2 < stages
    steps = PAIR * n_blk

    def copy(i, slot):
        return pltpu.make_async_copy(buf.at[slot], t.at[lax.div(i, n_blk), lax.rem(i, n_blk)], sems.at[slot])

    @pl.when(mine)
    def _():
        @pl.loop(0, steps)
        def _(i):
            slot = lax.rem(i, 2)

            @pl.when(i >= 2)
            def _():
                copy(i - 2, slot).wait()

            l = lax.div(i, n_blk)
            at = pl.ds(pl.multiple_of(lax.rem(i, n_blk) * blk, blk), blk)
            for j in range(n_blk):
                buf[slot, j * blk : (j + 1) * blk, :] = w[l, j, at, :].T
            copy(i, slot).start()

        copy(steps - 2, 0).wait()
        copy(steps - 1, 1).wait()


def forward_section(l, chunk, info, w, y, su, sx, sd, sr):
    n_blk, width, blk = w.shape[1:]
    inv = width ** (-0.5)
    xb = y[...]
    x = xb.astype(F32)
    scale = lax.rsqrt(jnp.mean(x * x, axis=-1, keepdims=True) + EPS)
    sx[l, chunk] = xb
    sr[l, chunk] = jnp.broadcast_to(scale, sr.shape[2:])
    su[l, chunk] = (x * scale).astype(BF16)

    @pl.loop(0, 2)
    def _(part):
        for i in range(n_blk // 2):
            j = part * (n_blk // 2) + i
            cols = pl.ds(pl.multiple_of(info[2 + j], blk), blk)
            z = dot(su[l, chunk], w[l, j]) * inv
            sg = jax.nn.sigmoid(z)
            sd[l, chunk, :, pl.ds(pl.multiple_of(j * blk, blk), blk)] = sg * (1.0 + z * (1.0 - sg)) * inv
            y[:, cols] = (sx[l, chunk, :, cols].astype(F32) + z * sg).astype(BF16)


def forward_kernel(tick, info, x_in, inp, w, su_i, sx_i, sd_i, sr_i, y, su, sx, sd, sr):
    del su_i, sx_i, sd_i, sr_i
    place = info[1]
    chunk = tick - SKEW * place

    @pl.when((chunk >= 0) & (chunk < CHUNKS))
    def _():
        @pl.when(place == 0)
        def _():
            y[...] = inp[chunk]

        @pl.when(place != 0)
        def _():
            y[...] = x_in[...]

        @pl.loop(0, PAIR)
        def _(l):
            forward_section(l, chunk, info, w, y, su, sx, sd, sr)


def start_kernel(info, inp, *refs):
    mine, other = refs[:8], refs[8:16]
    y, w, su, sx, sd, sr, sq, first, sems = refs[16:]
    del sq, first
    core = info[0]
    active = info[1] == 0

    def copies(slot, blocks):
        for i, block in enumerate(blocks):
            yield pltpu.make_async_copy(block, w.at[slot, pl.ds(2 * i, 2)], sems.at[slot, i])

    def start(slot):
        for here, blocks in ((core == slot, mine), (core != slot, other)):

            @pl.when(here)
            def _():
                for copy in copies(slot, blocks):
                    copy.start()

    @pl.when(active)
    def _():
        y[...] = inp[0]

    for slot in range(PAIR):
        start(slot)

    @pl.loop(0, PAIR)
    def _(l):
        for copy in copies(l, mine):
            copy.wait()

        @pl.when(active)
        def _():
            forward_section(l, 0, info, w, y, su, sx, sd, sr)


def backward_section(l, chunk, info, w, sx, sd, sr, dx, sq, qrel, du, acc):
    n_blk, width, blk = w.shape[1:]
    for j in range(n_blk):
        cols = pl.ds(pl.multiple_of(info[2 + j], blk), blk)
        q = (dx[:, cols].astype(F32) * sd[l, chunk, :, j * blk : (j + 1) * blk]).astype(BF16)
        qrel[:, j * blk : (j + 1) * blk] = q
        sq[l, chunk, :, cols] = q

    acc[...] = jnp.zeros_like(acc)
    scale = sr[l, chunk]

    @pl.loop(0, 2)
    def _(part):
        total = acc[...]
        for i in range(n_blk // 2):
            k = part * (n_blk // 2) + i
            cols = pl.ds(pl.multiple_of(k * blk, blk), blk)
            g = dot(qrel[...], w[l, k])
            du[:, cols] = g
            total = total + g * (sx[l, chunk, :, cols].astype(F32) * scale)
        acc[...] = total

    scale = scale[:, :1]
    n = sx[l, chunk].astype(F32) * scale
    mean = jnp.sum(acc[...], axis=-1, keepdims=True) * (1.0 / width)
    dx[...] = (dx[...].astype(F32) + scale * (du[...] - n * mean)).astype(BF16)


def backward_kernel(tick, stages, info, g_in, cot, w, sx, sd, sr, sq_i, dx, sq, qrel, du, acc):
    del sq_i
    place = stages - 1 - info[1]
    chunk = tick - SKEW * place

    @pl.when((chunk >= 0) & (chunk < CHUNKS))
    def _():
        @pl.when(place == 0)
        def _():
            dx[...] = cot[chunk]

        @pl.when(place != 0)
        def _():
            dx[...] = g_in[...]

        @pl.loop(0, PAIR)
        def _(step):
            backward_section(PAIR - 1 - step, chunk, info, w, sx, sd, sr, dx, sq, qrel, du, acc)


def turn_kernel(stages, info, cot, w_in, sx, sd, sr, sq_i, t, dx, sq, w, qrel, du, acc, sems):
    del w_in, sq_i
    half = w.shape[1] // 2

    def copies(l):
        for h in range(2):
            at = pl.ds(h * half, half)
            yield pltpu.make_async_copy(t.at[l, at], w.at[l, at], sems.at[l, h])

    for l in reversed(range(PAIR)):
        for copy in copies(l):
            copy.start()
    last = info[1] == stages - 1

    @pl.when(last)
    def _():
        dx[...] = cot[0]

    @pl.loop(0, PAIR)
    def _(step):
        l = PAIR - 1 - step
        for copy in copies(l):
            copy.wait()

        @pl.when(last)
        def _():
            backward_section(l, 0, info, w, sx, sd, sr, dx, sq, qrel, du, acc)


def pack_kernel(info, su, sq, out):
    other = 1 - info[0]
    out[0] = su[other]
    out[1] = sq[other]


def gradient_kernel(share, info, su, sq, recv, w_now, total, out, w_next):
    core = info[0]
    depth, width = out.shape
    cols = pl.ds(pl.multiple_of(pl.program_id(0) * depth, depth), depth)
    tokens = lambda v: v.reshape(-1, v.shape[-1])
    u = jnp.concatenate([tokens(su[core, :, :, cols]), tokens(recv[0, :, :, cols])], 0).T
    for k in range(0, width, 512):
        q = jnp.concatenate([tokens(sq[core, :, :, k : k + 512]), tokens(recv[1, :, :, k : k + 512])], 0)
        out[:, k : k + 512] = dot(u, q).astype(BF16)
    w_next[...] = w_now[...] - share * total[...].astype(F32)


VM = pl.BlockSpec(memory_space=pltpu.VMEM)
SM = pl.BlockSpec(memory_space=pltpu.SMEM)
HB = pl.BlockSpec(memory_space=pltpu.HBM)


def cost(flops):
    return pl.CostEstimate(flops=flops, bytes_accessed=0, transcendentals=0)


def params(mib):
    return pltpu.CompilerParams(vmem_limit_bytes=mib * 1024 * 1024)


def body(inputs, cotangent, w_prev, w_now, grads_prev):
    n_dp = lax.axis_size("dp")
    n_sec = lax.axis_size("section")
    stages = n_sec // PAIR
    _, tok_mb, width = inputs.shape
    blk = w_prev.shape[2]
    rows = tok_mb // CHUNKS
    sec = lax.axis_index("section")
    core = sec % PAIR
    stage = sec // PAIR
    dp = lax.axis_index("dp")
    n_y = n_dp // 2

    def over_dp(move):
        pairs = []
        for y in range(n_y):
            for z in range(2):
                ty, tz = move(y, z)
                pairs.append((2 * y + z, 2 * (ty % n_y) + tz))
        return lambda v: lax.ppermute(v, "dp", pairs)

    swap_z = over_dp(lambda y, z: (y, 1 - z))
    to_up = over_dp(lambda y, z: (y + 1, z))
    to_down = over_dp(lambda y, z: (y - 1, z))
    swap_core = lambda v: lax.ppermute(v, "section", [(s, s ^ 1) for s in range(n_sec)])

    lanes = blk // 2
    own = pl.pallas_call(
        round_kernel,
        grid=(4,),
        out_shape=jax.ShapeDtypeStruct((2, width, lanes), BF16),
        in_specs=[pl.BlockSpec((width // 4, blk), lambda i: (i, 0))],
        out_specs=pl.BlockSpec((2, width // 4, lanes), lambda i: (0, i, 0)),
        compiler_params=params(8),
        name="round",
    )(pltpu.with_memory_space_constraint(w_prev[0], pltpu.HBM))
    pick = lambda v, at: lax.dynamic_index_in_dim(v, at, 0, keepdims=False)
    inp = pick(inputs, core).reshape(CHUNKS, rows, width)
    cot = pick(cotangent, core).reshape(CHUNKS, rows, width)

    def swap_each(*values):
        swapped = []
        for v in values:
            if swapped:
                v, swapped[-1] = lax.optimization_barrier((v, swapped[-1]))
            swapped.append(swap_core(v))
        return swapped

    def linked(*moves):
        return [move(v) for move, v in moves]

    zo, below, above, own_o = lax.optimization_barrier(
        (*linked((swap_z, own), (to_up, own), (to_down, own)), *swap_each(own))
    )
    above, inp, cot = lax.optimization_barrier((above, inp, cot))
    above_z, below_z, far, zo_o, below_o, above_o = lax.optimization_barrier(
        (*linked((swap_z, above), (to_up, zo), (to_down, above)), *swap_each(zo, below, above))
    )
    far_za, far_zb, above_zo, below_zo, far_o = lax.optimization_barrier(
        (*linked((to_up, below_z[:1]), (to_down, above_z[1:])), *swap_each(above_z, below_z, far))
    )
    y_at, z_at = dp // 2, dp % 2
    rel = [(0, 0), (0, 1), (1, 0), (1, 1), (2, 0), (2, 1), (n_y - 1, 0), (n_y - 1, 1)]
    off = [(((y_at + dy) % n_y) * 2 + (z_at + dz) % 2) * blk + h * lanes for dy, dz in rel for h in range(2)]
    info = jnp.stack([core, stage] + off).astype(jnp.int32)
    far_z = jnp.concatenate([far_za, far_zb], 0)
    far_zo, gp, inp, cot, info_late = lax.optimization_barrier((swap_core(far_z), grads_prev, inp, cot, info))
    shares = lax.psum_scatter(gp[0, 0], "dp", scatter_dimension=1, tiled=True)

    saved = (PAIR, CHUNKS, rows, width)
    w_all = pltpu.VMEM((PAIR, 2 * n_dp, width, lanes), BF16)
    in_hbm = lambda *vs: [pltpu.with_memory_space_constraint(v, pltpu.HBM) for v in vs]
    info = info_late
    mine = (own, zo, above, above_z, far, far_z, below, below_z)
    other = (own_o, zo_o, above_o, above_zo, far_o, far_zo, below_o, below_zo)
    y_start, w_res, su, sx, sd, sr, sq, first = pl.pallas_call(
        start_kernel,
        out_shape=[
            pltpu.VMEM((rows, width), BF16),
            w_all,
            pltpu.VMEM(saved, BF16),
            pltpu.VMEM(saved, BF16),
            pltpu.VMEM(saved, F32),
            pltpu.VMEM((PAIR, CHUNKS, rows, 128), F32),
            pltpu.VMEM(saved, BF16),
            pltpu.VMEM((rows, width), BF16),
        ],
        in_specs=[SM, VM] + [HB] * 16,
        out_specs=[VM] * 8,
        scratch_shapes=[pltpu.SemaphoreType.DMA((PAIR, 8))],
        compiler_params=params(1),
        cost_estimate=cost(PAIR * 2 * rows * width * width),
        name="start",
    )(info, inp, *in_hbm(*mine, *other))

    def transposed(early, w, *t):
        return pl.pallas_call(
            functools.partial(transpose_kernel, early, stages),
            out_shape=pltpu.HBM(w.shape, w.dtype),
            in_specs=[SM, VM] + [HB] * len(t),
            out_specs=HB,
            input_output_aliases={2: 0} if t else {},
            scratch_shapes=[pltpu.VMEM((2, width, lanes), BF16), pltpu.SemaphoreType.DMA((2,))],
            compiler_params=params(2),
            name="transpose",
        )(info, w, *in_hbm(*t))

    def forward_call(tick, *args):
        return pl.pallas_call(
            functools.partial(forward_kernel, tick),
            out_shape=[
                pltpu.VMEM((rows, width), BF16),
                pltpu.VMEM(su.shape, su.dtype),
                pltpu.VMEM(sx.shape, sx.dtype),
                pltpu.VMEM(sd.shape, sd.dtype),
                pltpu.VMEM(sr.shape, sr.dtype),
            ],
            in_specs=[SM] + [VM] * 7,
            out_specs=[VM] * 5,
            input_output_aliases={4: 1, 5: 2, 6: 3, 7: 4},
            compiler_params=params(1),
            cost_estimate=cost(PAIR * 2 * rows * width * width),
            name="forward",
        )(info, *args)

    def backward_call(tick, *args):
        return pl.pallas_call(
            functools.partial(backward_kernel, tick, stages),
            out_shape=[pltpu.VMEM((rows, width), BF16), pltpu.VMEM(sq.shape, sq.dtype)],
            in_specs=[SM] + [VM] * 7,
            out_specs=[VM] * 2,
            scratch_shapes=[
                pltpu.VMEM((rows, width), BF16),
                pltpu.VMEM((rows, width), F32),
                pltpu.VMEM((rows, lanes), F32),
            ],
            input_output_aliases={7: 1},
            compiler_params=params(1),
            cost_estimate=cost(PAIR * 2 * rows * width * width),
            name="backward",
        )(info, *args)

    def turn_call(*args):
        return pl.pallas_call(
            functools.partial(turn_kernel, stages),
            out_shape=[pltpu.VMEM((rows, width), BF16), pltpu.VMEM(sq.shape, sq.dtype), w_all],
            in_specs=[SM] + [VM] * 6 + [HB],
            out_specs=[VM] * 3,
            scratch_shapes=[
                pltpu.VMEM((rows, width), BF16),
                pltpu.VMEM((rows, width), F32),
                pltpu.VMEM((rows, lanes), F32),
                pltpu.SemaphoreType.DMA((PAIR, 2)),
            ],
            input_output_aliases={6: 1, 2: 2},
            compiler_params=params(1),
            cost_estimate=cost(PAIR * 2 * rows * width * width),
            name="turn",
        )(info, *args)

    ticks = SKEW * (stages - 1) + CHUNKS

    def hop(value, tick, step):
        pairs = []
        for p in range(stages - 1):
            if 0 <= tick - SKEW * p < CHUNKS:
                a, b = (p, p + 1) if step > 0 else (stages - 1 - p, stages - 2 - p)
                pairs += [(PAIR * a + c, PAIR * b + c) for c in range(PAIR)]
        return lax.ppermute(value, "section", pairs) if pairs else None

    def relay(step, call):
        arrived = {}
        for tick in range(ticks):
            arrived[tick] = hop(call(tick, arrived.get(tick - SKEW)), tick, step)

    state = [w_res, su, sx, sd, sr, sq]
    flipped = []

    def forward(tick, arrived):
        if tick == 0:
            return y_start
        if tick in (1, SKEW * (stages // 2) + CHUNKS):
            flipped[:], state[1] = lax.optimization_barrier(([transposed(tick == 1, state[0], *flipped)], state[1]))
        x_in = first if arrived is None else arrived
        y, *state[1:5] = forward_call(tick, x_in, inp, *state[:5])
        return y

    def backward(tick, arrived):
        if tick == 0:
            g, state[5], state[0] = turn_call(cot, state[0], *state[2:6], *in_hbm(flipped[0]))
            return g
        g_in = first if arrived is None else arrived
        g, state[5] = backward_call(tick, g_in, cot, state[0], *state[2:6])
        return g

    relay(1, forward)
    relay(-1, backward)
    su, sq = state[1], state[5]

    packed = pl.pallas_call(
        pack_kernel,
        out_shape=pltpu.VMEM((2,) + saved[1:], BF16),
        in_specs=[SM, VM, VM],
        out_specs=VM,
        compiler_params=params(1),
        name="pack",
    )(info, su, sq)
    depth = 256
    row_block = lambda cols: pl.BlockSpec((depth, cols), lambda i: (i, 0))
    dweight, w_next = pl.pallas_call(
        functools.partial(gradient_kernel, LEARN_RATE / n_dp),
        grid=(width // depth,),
        out_shape=[jax.ShapeDtypeStruct((width, width), BF16), jax.ShapeDtypeStruct((width, blk), F32)],
        in_specs=[SM] + [VM] * 3 + [row_block(blk)] * 2,
        out_specs=[row_block(width), row_block(blk)],
        compiler_params=params(12),
        cost_estimate=cost(4 * tok_mb * width * width),
        name="gradient",
    )(info, su, sq, swap_core(packed), *in_hbm(w_now[0], shares))
    return (w_next[None], dweight[None, None])


def solution(mesh):
    placed = (
        P(None, "dp", None),
        P(None, "dp", None),
        P("section", None, "dp"),
        P("section", None, "dp"),
        P("dp", "section", None, None),
    )
    return jax.shard_map(
        body,
        mesh=mesh,
        in_specs=placed,
        out_specs=(P("section", None, "dp"), P("dp", "section", None, None)),
        check_vma=False,
    )
```
